32 devices in a mesh: grp: 16 (over z, x, core), tp: 2 (over y).
Axes of the slice: x: 2, y: 2, z: 4, core: 2. Of those that a mesh axis runs over, the one named last changes fastest.
Arguments:
- memory_rows: bfloat16 [16384, 4096], P('grp', 'tp'), may hold values from -24 to 24, as said below
- norm_gain: float32 [4096], replicated, may hold values from 0.25 to 1.75
- key_weight: bfloat16 [4096, 4096], P(None, 'tp'), may hold values from -0.09375 to 0.09375
- owner_table: int32 [2048], replicated, may hold values from 0 to 2047, as said below
Outputs:
- placed_keys: bfloat16 [16384, 4096], P('grp', 'tp')
The draws below stay inside these ranges and needn't reach their ends.
Inputs may be any that keep to these rules, and one draw needn't show every extreme that they name: A permutation of the 2048 block numbers. Block b of the input goes to block position owner_table[b], which lies in group owner_table[b] // 128. The 128 blocks of one group go to all 16 groups, exactly 8 blocks to each of them. `memory_rows`: rows have offsets and scales of their own, and features a common pattern.
All inputs are finite; a program needn't handle non-finite values.
Results may differ from the reference program's by a relative error of at most 0.0049.
Values may be sent and summed in bfloat16 or wider, within the bound.
A program may use at most 64 MiB of HBM per device.

```python
import jax
import jax.numpy as jnp
from jax import lax

D = 4096
BLK_ROWS = 8
BLK_DEV = 128
ROWS = 16384
NB = 2048


def draw_memory_rows(key, part):
    key_off, key_scale, key_noise, key_pattern = jax.random.split(key, 4)
    offsets = jax.random.uniform(key_off, (ROWS, 1), jnp.float32, -1.5, 1.5)
    pattern = jnp.clip(jax.random.normal(key_pattern, (1, D), jnp.float32), -3.0, 3.0)
    scales = jnp.exp(jax.random.uniform(key_scale, (ROWS, 1), jnp.float32, jnp.log(0.5), jnp.log(3.0)))
    noise = jnp.clip(jax.random.normal(key_noise, (ROWS, D), jnp.float32), -4.0, 4.0)
    values = offsets + scales * (noise + 0.7 * pattern)
    return jnp.clip(values, -24.0, 24.0).astype(jnp.bfloat16)


def draw_owner_table(key, part):
    groups = NB // BLK_DEV
    per_pair = BLK_DEV // groups
    key_tau, key_offs, key_cols, key_slots = jax.random.split(key, 4)
    shuffle = jax.random.permutation(key_tau, groups).astype(jnp.int32)
    offsets = jax.random.permutation(key_offs, groups).astype(jnp.int32)
    column_keys = jax.random.split(key_cols, groups)
    column_perm = jax.vmap(lambda one_key: jax.random.permutation(one_key, BLK_DEV))(column_keys).astype(jnp.int32)
    sources = jnp.arange(groups, dtype=jnp.int32)[:, None]
    target = shuffle[(sources + offsets[column_perm % groups]) % groups]
    arrival = sources * per_pair + column_perm // groups
    slot_keys = jax.random.split(key_slots, groups)
    slot_perm = jax.vmap(lambda one_key: jax.random.permutation(one_key, BLK_DEV))(slot_keys).astype(jnp.int32)
    slots = slot_perm[target, arrival]
    return (target * BLK_DEV + slots).reshape(-1).astype(jnp.int32)


def level_of(own_key, extent, cuts, low, high):
    def one(axis_at, blocks):
        draws = jax.random.uniform(jax.random.fold_in(jax.random.fold_in(own_key, 6), axis_at), (blocks,), jnp.float32, low / len(cuts), high / len(cuts))
        return jnp.repeat(jnp.exp(draws), extent[axis_at] // blocks).reshape((-1,) + (1,) * (len(extent) - axis_at - 1))

    factor_of = one(*cuts[0])
    for cut in cuts[1:]:
        factor_of = factor_of * one(*cut)
    return factor_of


def normal_values(rng, dims, width, reach, cuts=(), kind=jnp.bfloat16):
    values = jax.random.normal(rng, dims, jnp.float32) * width
    if len(cuts) > 0:
        values = level_of(rng, dims, cuts, -0.22, 0.18) * values
    return jnp.clip(values, min=-reach, max=reach).astype(kind)


def setup_inputs(seed: int = 0) -> dict:
    arg_keys = jax.random.split(jax.random.key(seed), 5)
    memory_rows = draw_memory_rows(jax.random.fold_in(arg_keys[4], 71), 0)
    norm_gain = jnp.clip(1.0 + 0.15 * jax.random.normal(arg_keys[1], (D,), jnp.float32), 0.25, 1.75)
    key_weight = normal_values(arg_keys[2], (D, D), D ** -0.5, 0.09375, ((1, 2),))
    owner_table = draw_owner_table(jax.random.fold_in(arg_keys[4], 71), 0)
    return dict(memory_rows=memory_rows, norm_gain=norm_gain, key_weight=key_weight, owner_table=owner_table)


EPS = 1e-05

def reference(memory_rows, norm_gain, key_weight, owner_table):
    values = memory_rows.astype(jnp.float32)
    row_sum = lax.optimization_barrier(jnp.sum(values, axis=1, keepdims=True))
    row_sq = lax.optimization_barrier(jnp.sum(values * values, axis=1, keepdims=True))
    row_mean = row_sum / D
    row_var = row_sq / D - row_mean * row_mean
    normed = ((values - row_mean) * lax.rsqrt(row_var + EPS) * norm_gain[None, :]).astype(jnp.bfloat16)
    keys = jnp.dot(normed, key_weight, preferred_element_type=jnp.float32).astype(jnp.bfloat16)
    blocks = keys.reshape(NB, BLK_ROWS, D)
    placed = jnp.zeros_like(blocks).at[owner_table.astype(jnp.int32)].set(blocks)
    return placed.reshape(ROWS, D)
```

```python
import functools

import jax
import jax.numpy as jnp
from jax import lax
from jax.experimental import pallas as pl
from jax.experimental.pallas import tpu as pltpu
from jax.sharding import PartitionSpec as P

BLK_ROWS = 8
EPS = 1e-05
CHUNKS = 8
MIB = 1024 * 1024
MESH = pl.DeviceIdType.MESH


def flipped(me, mask, groups):
    out = me
    bit = 1
    while bit < groups:
        out = out + ((mask // bit) % 2) * bit * (1 - 2 * ((me // bit) % 2))
        bit *= 2
    return out


def sort_kernel(groups, table_ref, rows_ref, out_ref, count_ref, sem):
    me = lax.axis_index("grp")
    blocks = rows_ref.shape[0]
    capacity = blocks // groups

    def clear(g, carry):
        count_ref[g] = 0
        return carry

    lax.fori_loop(0, groups, clear, 0)

    def move(b, carry):
        target = table_ref[me * blocks + b] // blocks
        rank = count_ref[target]
        count_ref[target] = rank + 1
        step = groups - 1 - (me ^ target)
        pltpu.make_async_copy(rows_ref.at[b], out_ref.at[step * capacity + rank], sem).start()
        return carry

    lax.fori_loop(0, blocks, move, 0)
    pltpu.make_async_copy(rows_ref, out_ref, sem).wait()


def place_kernel(groups, slot_ref, in_ref, out_ref, sem):
    me = lax.axis_index("grp")
    blocks = in_ref.shape[0]
    capacity = blocks // groups

    def move(i, carry):
        step = i // capacity
        source = me ^ (groups - 1 - step)
        slot = slot_ref[source, i - step * capacity]
        pltpu.make_async_copy(in_ref.at[i], out_ref.at[slot], sem).start()
        return carry

    lax.fori_loop(0, blocks, move, 0)
    pltpu.make_async_copy(in_ref, out_ref, sem).wait()


def main_kernel(
    groups, parts, rows_ref, gain_ref, weight_ref, out_ref,
    mine, others, weight, keys, normed, gains,
    mine_sem, weight_sem, gain_sem, gather_send, gather_recv, key_send, key_recv, self_sem,
):
    me = lax.axis_index("grp")
    part = lax.axis_index("tp")
    row_count, depth = rows_ref.shape
    width = depth * parts
    chunk = row_count // CHUNKS
    per_chunk = groups // CHUNKS
    piece = row_count // groups

    barrier = pltpu.get_barrier_semaphore()
    for j in range(1, parts):
        pl.semaphore_signal(
            barrier, inc=1, device_id={"tp": (part + j) % parts}, device_id_type=MESH
        )

    def greet(mask, carry):
        pl.semaphore_signal(
            barrier, inc=1, device_id={"grp": flipped(me, mask, groups)}, device_id_type=MESH
        )
        return carry

    lax.fori_loop(1, groups, greet, 0)

    def own_copy(c):
        at = pl.ds(c * chunk, chunk)
        return pltpu.make_async_copy(rows_ref.at[at], mine.at[at], mine_sem.at[c])

    def weight_copy(j):
        origin = (part + j) % parts
        return pltpu.make_async_copy(
            weight_ref.at[pl.ds(pl.multiple_of(origin * depth, depth), depth)],
            weight.at[pl.ds(j * depth, depth)],
            weight_sem.at[j],
        )

    def gain_copy(j):
        origin = (part + j) % parts
        return pltpu.make_async_copy(
            gain_ref.at[:, pl.ds(pl.multiple_of(origin * depth, depth), depth)],
            gains.at[:, pl.ds(j * depth, depth)],
            gain_sem.at[j],
        )

    def gather_copy(c, j):
        at = pl.ds(c * chunk, chunk)
        return pltpu.make_async_remote_copy(
            src_ref=rows_ref.at[at],
            dst_ref=others.at[j - 1, at],
            send_sem=gather_send.at[j - 1, c],
            recv_sem=gather_recv.at[j - 1, c],
            device_id={"tp": (part + parts - j) % parts},
            device_id_type=MESH,
        )

    def key_copy(step):
        at = pl.ds(step * piece, piece)
        return pltpu.make_async_remote_copy(
            src_ref=keys.at[at],
            dst_ref=out_ref.at[at],
            send_sem=key_send.at[step],
            recv_sem=key_recv.at[step],
            device_id={"grp": flipped(me, groups - 1 - step, groups)},
            device_id_type=MESH,
        )

    def self_copy():
        at = pl.ds((groups - 1) * piece, piece)
        return pltpu.make_async_copy(keys.at[at], out_ref.at[at], self_sem)

    for j in range(parts):
        gain_copy(j).start()
        weight_copy(j).start()
    for c in range(CHUNKS):
        own_copy(c).start()
    pl.semaphore_wait(barrier, groups - 1 + parts - 1)
    for c in range(CHUNKS):
        for j in range(1, parts):
            gather_copy(c, j).start()
    for j in range(parts):
        gain_copy(j).wait()
        weight_copy(j).wait()

    sub = 2 * BLK_ROWS
    tile = depth // 4

    def one_chunk(c, carry):
        base = pl.multiple_of(c * chunk, chunk)
        own_copy(c).wait()
        for j in range(1, parts):
            gather_copy(c, j).wait_recv()

        def norm_rows(i, carry):
            at = pl.ds(pl.multiple_of(base + i * sub, sub), sub)
            to = pl.ds(pl.multiple_of(i * sub, sub), sub)

            def values(j):
                held = mine[at, :] if j == 0 else others[j - 1, at, :]
                return held.astype(jnp.float32)

            row_sum = 0.0
            row_sq = 0.0
            for j in range(parts):
                x = values(j)
                row_sum = row_sum + jnp.sum(x, axis=1, keepdims=True)
                row_sq = row_sq + jnp.sum(x * x, axis=1, keepdims=True)
            mean = row_sum / width
            scale = lax.rsqrt(row_sq / width - mean * mean + EPS)
            for j in range(parts):
                cols = pl.ds(j * depth, depth)
                normed[to, cols] = ((values(j) - mean) * scale * gains[:, cols]).astype(
                    jnp.bfloat16
                )
            return carry

        lax.fori_loop(0, chunk // sub, norm_rows, 0)

        def columns(n, carry):
            cols = pl.ds(pl.multiple_of(n * tile, tile), tile)
            keys[pl.ds(base, chunk), cols] = jnp.dot(
                normed[...], weight[:, cols], preferred_element_type=jnp.float32
            ).astype(jnp.bfloat16)
            return carry

        lax.fori_loop(0, keys.shape[1] // tile, columns, 0)

        for i in range(per_chunk):
            step = c * per_chunk + i
            if i < per_chunk - 1:
                key_copy(step).start()
            else:
                @pl.when(c < CHUNKS - 1)
                def _():
                    key_copy(step).start()

                @pl.when(c == CHUNKS - 1)
                def _():
                    self_copy().start()
        return carry

    lax.fori_loop(0, CHUNKS, one_chunk, 0)

    for c in range(CHUNKS):
        for j in range(1, parts):
            gather_copy(c, j).wait_send()

    def finish(step, carry):
        key_copy(step).wait()
        return carry

    lax.fori_loop(0, groups - 1, finish, 0)
    self_copy().wait()


def on_device(groups, parts, memory_rows, norm_gain, key_weight, owner_table):
    row_count, depth = memory_rows.shape
    columns = key_weight.shape[1]
    blocks = row_count // BLK_ROWS
    capacity = blocks // groups
    position = lax.axis_index("grp")
    any_space = pl.BlockSpec(memory_space=pl.ANY)
    in_vmem = pl.BlockSpec(memory_space=pltpu.VMEM)
    in_smem = pl.BlockSpec(memory_space=pltpu.SMEM)

    in_order = pl.pallas_call(
        functools.partial(sort_kernel, groups),
        out_shape=jax.ShapeDtypeStruct((blocks, BLK_ROWS, depth), jnp.bfloat16),
        in_specs=[in_smem, any_space],
        out_specs=in_vmem,
        scratch_shapes=[pltpu.SMEM((groups,), jnp.int32), pltpu.SemaphoreType.DMA],
        compiler_params=pltpu.CompilerParams(vmem_limit_bytes=16 * MIB),
        name="sort",
    )(owner_table, memory_rows.reshape(blocks, BLK_ROWS, depth))

    table = owner_table.reshape(groups, blocks)
    to_me = table // blocks == position
    lower = jnp.triu(jnp.ones((blocks, blocks), jnp.bfloat16), 1)
    rank = jnp.dot(to_me.astype(jnp.bfloat16), lower, preferred_element_type=jnp.float32)
    rank = jnp.where(to_me, rank.astype(jnp.int32), -1)
    wanted = jnp.arange(capacity, dtype=jnp.int32)[None, :, None]
    slots = jnp.sum(jnp.where(rank[:, None, :] == wanted, (table % blocks)[:, None, :], 0), axis=2)

    dma = pltpu.SemaphoreType.DMA
    incoming = pl.pallas_call(
        functools.partial(main_kernel, groups, parts),
        out_shape=jax.ShapeDtypeStruct((row_count, columns), jnp.bfloat16),
        in_specs=[any_space, any_space, any_space],
        out_specs=any_space,
        scratch_shapes=[
            pltpu.VMEM((row_count, depth), jnp.bfloat16),
            pltpu.VMEM((parts - 1, row_count, depth), jnp.bfloat16),
            pltpu.VMEM((depth * parts, columns), jnp.bfloat16),
            pltpu.VMEM((row_count, columns), jnp.bfloat16),
            pltpu.VMEM((row_count // CHUNKS, depth * parts), jnp.bfloat16),
            pltpu.VMEM((1, depth * parts), jnp.float32),
            dma((CHUNKS,)),
            dma((parts,)),
            dma((parts,)),
            dma((parts - 1, CHUNKS)),
            dma((parts - 1, CHUNKS)),
            dma((groups,)),
            dma((groups,)),
            dma,
        ],
        compiler_params=pltpu.CompilerParams(
            collective_id=0, has_side_effects=True, vmem_limit_bytes=48 * MIB
        ),
        name="exchange",
    )(in_order.reshape(row_count, depth), norm_gain[None, :], key_weight)

    placed = pl.pallas_call(
        functools.partial(place_kernel, groups),
        out_shape=jax.ShapeDtypeStruct((blocks, BLK_ROWS, columns), jnp.bfloat16),
        in_specs=[in_smem, in_vmem],
        out_specs=any_space,
        scratch_shapes=[pltpu.SemaphoreType.DMA],
        compiler_params=pltpu.CompilerParams(vmem_limit_bytes=16 * MIB),
        name="place",
    )(slots, incoming.reshape(blocks, BLK_ROWS, columns))
    return placed.reshape(row_count, columns)


def solution(mesh):
    in_specs = (P("grp", "tp"), P(), P(None, "tp"), P())
    out_specs = P("grp", "tp")
    return jax.shard_map(
        functools.partial(on_device, mesh.shape["grp"], mesh.shape["tp"]),
        mesh=mesh, in_specs=in_specs, out_specs=out_specs, check_vma=False,
    )
```

```python
import functools

import jax
import jax.numpy as jnp
from jax import lax
from jax.experimental import pallas as pl
from jax.experimental.pallas import tpu as pltpu
from jax.sharding import PartitionSpec as P

BLK_ROWS = 8
EPS = 1e-05
CHUNKS = 16
MIB = 1024 * 1024
MESH = pl.DeviceIdType.MESH


def flipped(me, mask, groups):
    out = me
    bit = 1
    while bit < groups:
        out = out + ((mask // bit) % 2) * bit * (1 - 2 * ((me // bit) % 2))
        bit *= 2
    return out


def mask_at(me, step, groups):
    quarter = groups // 4
    inner = ((me // quarter + 1) // 2) % 2
    turn = step // quarter
    first = (3 - turn) // 3
    second = (turn % 2) * (1 - turn // 2)
    third = (turn // 2) * (1 - turn % 2)
    far = first * (1 + inner) + 3 * second + third * (2 - inner)
    return far * quarter + quarter - 1 - step % quarter


def place_kernel(groups, slot_ref, in_ref, out_ref, sem):
    me = lax.axis_index("grp")
    blocks = in_ref.shape[0]
    capacity = blocks // groups

    def move(i, carry):
        mask = i // capacity
        slot = slot_ref[me ^ mask, i - mask * capacity]
        pltpu.make_async_copy(in_ref.at[i], out_ref.at[slot], sem).start()
        return carry

    lax.fori_loop(0, blocks, move, 0)
    pltpu.make_async_copy(in_ref, out_ref, sem).wait()


def main_kernel(
    groups, parts, index_ref, rows_ref, gain_ref, weight_ref, out_ref,
    raw, mine, others, weight, keys, normed, gains,
    raw_sem, weight_sem, gain_sem, gather_send, gather_recv, key_send, key_recv, self_sem,
):
    me = lax.axis_index("grp")
    part = lax.axis_index("tp")
    blocks, _, depth = rows_ref.shape
    row_count = blocks * BLK_ROWS
    width = depth * parts
    chunk = row_count // CHUNKS
    chunk_blocks = blocks // CHUNKS
    capacity = blocks // groups
    per_chunk = groups // CHUNKS
    piece = row_count // groups

    barrier = pltpu.get_barrier_semaphore()
    for j in range(1, parts):
        pl.semaphore_signal(
            barrier, inc=1, device_id={"tp": (part + j) % parts}, device_id_type=MESH
        )

    def greet(mask, carry):
        pl.semaphore_signal(
            barrier, inc=1, device_id={"grp": flipped(me, mask, groups)}, device_id_type=MESH
        )
        return carry

    lax.fori_loop(1, groups, greet, 0)

    raw_copy = pltpu.make_async_copy(rows_ref, raw, raw_sem)

    def weight_copy(j):
        origin = (part + j) % parts
        return pltpu.make_async_copy(
            weight_ref.at[pl.ds(pl.multiple_of(origin * depth, depth), depth)],
            weight.at[pl.ds(j * depth, depth)],
            weight_sem.at[j],
        )

    def gain_copy(j):
        origin = (part + j) % parts
        return pltpu.make_async_copy(
            gain_ref.at[:, pl.ds(pl.multiple_of(origin * depth, depth), depth)],
            gains.at[:, pl.ds(j * depth, depth)],
            gain_sem.at[j],
        )

    def gather_copy(c, j):
        at = pl.ds(c * chunk_blocks, chunk_blocks)
        return pltpu.make_async_remote_copy(
            src_ref=mine.at[at],
            dst_ref=others.at[j - 1, at],
            send_sem=gather_send.at[j - 1, c],
            recv_sem=gather_recv.at[j - 1, c],
            device_id={"tp": (part + parts - j) % parts},
            device_id_type=MESH,
        )

    def key_copy(step):
        mask = mask_at(me, step, groups)
        return pltpu.make_async_remote_copy(
            src_ref=keys.at[pl.ds(step * piece, piece)],
            dst_ref=out_ref.at[pl.ds(mask * piece, piece)],
            send_sem=key_send.at[step],
            recv_sem=key_recv.at[mask],
            device_id={"grp": flipped(me, mask, groups)},
            device_id_type=MESH,
        )

    def self_copy():
        at = pl.ds((groups - 1) * piece, piece)
        return pltpu.make_async_copy(keys.at[at], out_ref.at[pl.ds(0, piece)], self_sem)

    raw_copy.start()
    for j in range(parts):
        gain_copy(j).start()
        weight_copy(j).start()
    raw_copy.wait()

    def arrange(c):
        def take(i, carry):
            step = i // capacity
            mine[i] = raw[index_ref[groups + step, i - step * capacity]]
            return carry

        lax.fori_loop(c * chunk_blocks, (c + 1) * chunk_blocks, take, 0)

    arrange(0)
    pl.semaphore_wait(barrier, groups - 1 + parts - 1)
    for c in range(CHUNKS):
        if c > 0:
            arrange(c)
        for j in range(1, parts):
            gather_copy(c, j).start()
    for j in range(parts):
        gain_copy(j).wait()
        weight_copy(j).wait()

    sub = 2 * BLK_ROWS
    tile = depth // 4

    def one_chunk(c, carry):
        base = pl.multiple_of(c * chunk, chunk)
        for j in range(1, parts):
            gather_copy(c, j).wait_recv()

        def norm_rows(i, carry):
            at = pl.ds(c * chunk_blocks + i * 2, 2)
            to = pl.ds(pl.multiple_of(i * sub, sub), sub)

            def values(j):
                held = mine[at] if j == 0 else others[j - 1, at]
                return held.astype(jnp.float32).reshape(sub, depth)

            row_sum = 0.0
            row_sq = 0.0
            for j in range(parts):
                x = values(j)
                row_sum = row_sum + jnp.sum(x, axis=1, keepdims=True)
                row_sq = row_sq + jnp.sum(x * x, axis=1, keepdims=True)
            mean = row_sum / width
            scale = lax.rsqrt(row_sq / width - mean * mean + EPS)
            for j in range(parts):
                cols = pl.ds(j * depth, depth)
                normed[to, cols] = ((values(j) - mean) * scale * gains[:, cols]).astype(
                    jnp.bfloat16
                )
            return carry

        lax.fori_loop(0, chunk // sub, norm_rows, 0)

        def columns(n, carry):
            cols = pl.ds(pl.multiple_of(n * tile, tile), tile)
            keys[pl.ds(base, chunk), cols] = jnp.dot(
                normed[...], weight[:, cols], preferred_element_type=jnp.float32
            ).astype(jnp.bfloat16)
            return carry

        lax.fori_loop(0, keys.shape[1] // tile, columns, 0)

        for i in range(per_chunk):
            step = c * per_chunk + i
            if i < per_chunk - 1:
                key_copy(step).start()
            else:
                @pl.when(c < CHUNKS - 1)
                def _():
                    key_copy(step).start()

                @pl.when(c == CHUNKS - 1)
                def _():
                    self_copy().start()
        return carry

    lax.fori_loop(0, CHUNKS, one_chunk, 0)

    for c in range(CHUNKS):
        for j in range(1, parts):
            gather_copy(c, j).wait_send()

    def finish(step, carry):
        key_copy(step).wait()
        return carry

    lax.fori_loop(0, groups - 1, finish, 0)
    self_copy().wait()


def on_device(groups, parts, memory_rows, norm_gain, key_weight, owner_table):
    row_count, depth = memory_rows.shape
    columns = key_weight.shape[1]
    blocks = row_count // BLK_ROWS
    capacity = blocks // groups
    position = lax.axis_index("grp")
    any_space = pl.BlockSpec(memory_space=pl.ANY)
    in_vmem = pl.BlockSpec(memory_space=pltpu.VMEM)
    in_smem = pl.BlockSpec(memory_space=pltpu.SMEM)

    table = owner_table.reshape(groups, blocks)
    own = lax.dynamic_slice_in_dim(table, position, 1, axis=0)
    steps = jnp.arange(groups, dtype=jnp.int32)
    peers = position ^ mask_at(position, steps, groups)
    chosen = jnp.concatenate([table // blocks == position, own // blocks == peers[:, None]])
    block_ids = jnp.broadcast_to(jnp.arange(blocks, dtype=jnp.int32)[None], table.shape)
    values = jnp.concatenate([table % blocks, block_ids])
    lower = jnp.triu(jnp.ones((blocks, blocks), jnp.bfloat16), 1)
    rank = jnp.dot(chosen.astype(jnp.bfloat16), lower, preferred_element_type=jnp.float32)
    rank = jnp.where(chosen, rank.astype(jnp.int32), -1)
    wanted = jnp.arange(capacity, dtype=jnp.int32)[None, :, None]
    index = jnp.sum(jnp.where(rank[:, None, :] == wanted, values[:, None, :], 0), axis=2)

    dma = pltpu.SemaphoreType.DMA
    incoming = pl.pallas_call(
        functools.partial(main_kernel, groups, parts),
        out_shape=jax.ShapeDtypeStruct((row_count, columns), jnp.bfloat16),
        in_specs=[in_smem, any_space, any_space, any_space],
        out_specs=any_space,
        scratch_shapes=[
            pltpu.VMEM((blocks, BLK_ROWS, depth), jnp.bfloat16),
            pltpu.VMEM((blocks, BLK_ROWS, depth), jnp.bfloat16),
            pltpu.VMEM((parts - 1, blocks, BLK_ROWS, depth), jnp.bfloat16),
            pltpu.VMEM((depth * parts, columns), jnp.bfloat16),
            pltpu.VMEM((row_count, columns), jnp.bfloat16),
            pltpu.VMEM((row_count // CHUNKS, depth * parts), jnp.bfloat16),
            pltpu.VMEM((1, depth * parts), jnp.float32),
            dma,
            dma((parts,)),
            dma((parts,)),
            dma((parts - 1, CHUNKS)),
            dma((parts - 1, CHUNKS)),
            dma((groups,)),
            dma((groups,)),
            dma,
        ],
        compiler_params=pltpu.CompilerParams(
            collective_id=0, has_side_effects=True, vmem_limit_bytes=48 * MIB
        ),
        name="exchange",
    )(index, memory_rows.reshape(blocks, BLK_ROWS, depth), norm_gain[None, :], key_weight)

    placed = pl.pallas_call(
        functools.partial(place_kernel, groups),
        out_shape=jax.ShapeDtypeStruct((blocks, BLK_ROWS, columns), jnp.bfloat16),
        in_specs=[in_smem, in_vmem],
        out_specs=any_space,
        scratch_shapes=[pltpu.SemaphoreType.DMA],
        compiler_params=pltpu.CompilerParams(vmem_limit_bytes=16 * MIB),
        name="place",
    )(index, incoming.reshape(blocks, BLK_ROWS, columns))
    return placed.reshape(row_count, columns)


def solution(mesh):
    in_specs = (P("grp", "tp"), P(), P(None, "tp"), P())
    out_specs = P("grp", "tp")
    return jax.shard_map(
        functools.partial(on_device, mesh.shape["grp"], mesh.shape["tp"]),
        mesh=mesh, in_specs=in_specs, out_specs=out_specs, check_vma=False,
    )
```

```python
import functools

import jax
import jax.numpy as jnp
from jax import lax
from jax.experimental import pallas as pl
from jax.experimental.pallas import tpu as pltpu
from jax.sharding import PartitionSpec as P

BLK_ROWS = 8
EPS = 1e-05
CHUNKS = 16
MIB = 1024 * 1024
MESH = pl.DeviceIdType.MESH


def flipped(me, mask, groups):
    out = me
    bit = 1
    while bit < groups:
        out = out + ((mask // bit) % 2) * bit * (1 - 2 * ((me // bit) % 2))
        bit *= 2
    return out


def mask_at(me, step, groups):
    quarter = groups // 4
    inner = ((me // quarter + 1) // 2) % 2
    turn = step // quarter
    first = (3 - turn) // 3
    second = (turn % 2) * (1 - turn // 2)
    third = (turn // 2) * (1 - turn % 2)
    far = first * (1 + inner) + 3 * second + third * (2 - inner)
    return far * quarter + quarter - 1 - step % quarter


def peer_mask(me, step, groups, early):
    regular = groups - early
    split = groups // 2 - early
    is_early = step // regular
    after = (1 + step // split) // 2
    late = step - regular + split
    return mask_at(me, is_early * late + (1 - is_early) * (step + early * after), groups)


def index_kernel(groups, per_chunk, table_ref, slot_ref, index_ref):
    me = lax.axis_index("grp")
    blocks = table_ref.shape[1]
    capacity = blocks // groups

    lane = lax.broadcasted_iota(jnp.int32, (groups, blocks), 1)
    row = lax.broadcasted_iota(jnp.int32, (groups, blocks), 0)
    peer = jnp.zeros((groups, blocks), jnp.int32)
    for step in range(groups):
        mask = peer_mask(me, step, groups, per_chunk)
        peer = jnp.where(row == step, flipped(me, mask, groups), peer)

    def ranked(offset, value):
        chosen = (offset >= 0) & (offset < blocks)
        counted = chosen.astype(jnp.int32)
        shift = 1
        while shift < blocks:
            counted = counted + jnp.where(lane >= shift, pltpu.roll(counted, shift, 1), 0)
            shift *= 2
        result = jnp.zeros((groups, blocks), jnp.int32)
        for r in range(capacity):
            at_rank = jnp.where(chosen & (counted == r + 1), value, 0).astype(jnp.float32)
            found = jnp.sum(at_rank, axis=1, keepdims=True).astype(jnp.int32)
            result = jnp.where(lane == r, found, result)
        return result

    own = jnp.broadcast_to(table_ref[pl.ds(me, 1), :], (groups, blocks))
    index_ref[...] = ranked(own - peer * blocks, lane)
    offset = table_ref[...] - me * blocks
    slot_ref[...] = ranked(offset, offset)


def place_kernel(groups, slot_ref, in_ref, out_ref, sem):
    me = lax.axis_index("grp")
    blocks = in_ref.shape[0]
    capacity = blocks // groups

    def move(i, carry):
        mask = i // capacity
        slot = slot_ref[me ^ mask, i - mask * capacity]
        pltpu.make_async_copy(in_ref.at[i], out_ref.at[slot], sem).start()
        return carry

    lax.fori_loop(0, blocks, move, 0)
    pltpu.make_async_copy(in_ref, out_ref, sem).wait()


def main_kernel(
    groups, parts, index_ref, rows_ref, gain_ref, weight_ref, out_ref,
    raw, away, mine, others, weight, keys, normed, gains,
    raw_sem, early_send, early_recv, weight_sem, gain_sem, gather_send, gather_recv, key_send, key_recv, self_sem,
):
    me = lax.axis_index("grp")
    part = lax.axis_index("tp")
    blocks, _, depth = rows_ref.shape
    row_count = blocks * BLK_ROWS
    width = depth * parts
    chunk = row_count // CHUNKS
    chunk_blocks = blocks // CHUNKS
    capacity = blocks // groups
    per_chunk = groups // CHUNKS
    piece = row_count // groups
    regular = groups - per_chunk

    barrier = pltpu.get_barrier_semaphore()
    for j in range(1, parts):
        pl.semaphore_signal(
            barrier, inc=1, device_id={"tp": (part + j) % parts}, device_id_type=MESH
        )

    def greet(mask, carry):
        pl.semaphore_signal(
            barrier, inc=1, device_id={"grp": flipped(me, mask, groups)}, device_id_type=MESH
        )
        return carry

    lax.fori_loop(1, groups, greet, 0)

    raw_copy = pltpu.make_async_copy(rows_ref, raw, raw_sem)

    def weight_copy(j):
        origin = (part + j) % parts
        return pltpu.make_async_copy(
            weight_ref.at[pl.ds(pl.multiple_of(origin * depth, depth), depth)],
            weight.at[pl.ds(j * depth, depth)],
            weight_sem.at[j],
        )

    def gain_copy(j):
        origin = (part + j) % parts
        return pltpu.make_async_copy(
            gain_ref.at[:, pl.ds(pl.multiple_of(origin * depth, depth), depth)],
            gains.at[:, pl.ds(j * depth, depth)],
            gain_sem.at[j],
        )

    def gather_copy(c, j):
        at = pl.ds(c * chunk_blocks, chunk_blocks)
        return pltpu.make_async_remote_copy(
            src_ref=mine.at[at],
            dst_ref=others.at[j - 1, at],
            send_sem=gather_send.at[j - 1, c],
            recv_sem=gather_recv.at[j - 1, c],
            device_id={"tp": (part + parts - j) % parts},
            device_id_type=MESH,
        )

    def key_copy(step):
        mask = peer_mask(me, step, groups, per_chunk)
        return pltpu.make_async_remote_copy(
            src_ref=keys.at[pl.ds(step * piece, piece)],
            dst_ref=out_ref.at[pl.ds(mask * piece, piece)],
            send_sem=key_send.at[step],
            recv_sem=key_recv.at[mask],
            device_id={"grp": flipped(me, mask, groups)},
            device_id_type=MESH,
        )

    def local_copy(i):
        step = regular + i if i < per_chunk else regular - 1
        mask = peer_mask(me, step, groups, per_chunk)
        return pltpu.make_async_copy(
            keys.at[pl.ds(step * piece, piece)],
            out_ref.at[pl.ds(mask * piece, piece)],
            self_sem.at[i],
        )

    def early_copy(i):
        mask = peer_mask(me, regular + i, groups, per_chunk)
        return pltpu.make_async_remote_copy(
            src_ref=away.at[pl.ds(i * capacity, capacity)],
            dst_ref=mine.at[pl.ds((regular + i) * capacity, capacity)],
            send_sem=early_send.at[i],
            recv_sem=early_recv.at[i],
            device_id={"grp": flipped(me, mask, groups)},
            device_id_type=MESH,
        )

    raw_copy.start()

    for j in range(parts):
        gain_copy(j).start()
    raw_copy.wait()
    for j in range(parts):
        weight_copy(j).start()

    def arrange(c):
        def take(i, carry):
            step = i // capacity
            block = raw[index_ref[step, i - step * capacity]]
            if c == CHUNKS - 1:
                away[i - c * chunk_blocks] = block
            else:
                mine[i] = block
            return carry

        lax.fori_loop(c * chunk_blocks, (c + 1) * chunk_blocks, take, 0)

    arrange(CHUNKS - 1)
    arrange(0)
    pl.semaphore_wait(barrier, groups - 1 + parts - 1)
    for i in range(per_chunk):
        early_copy(i).start()
    for c in range(CHUNKS - 1):
        if c > 0:
            arrange(c)
        for j in range(1, parts):
            gather_copy(c, j).start()
    for j in range(parts):
        gain_copy(j).wait()
        weight_copy(j).wait()

    sub = 2 * BLK_ROWS
    tile = depth // 4

    def one_chunk(c, carry):
        base = pl.multiple_of(c * chunk, chunk)

        @pl.when(c == CHUNKS // 2)
        def _():
            for i in range(per_chunk):
                early_copy(i).wait_recv()
            for j in range(1, parts):
                gather_copy(CHUNKS - 1, j).start()

        for j in range(1, parts):
            gather_copy(c, j).wait_recv()

        def norm_rows(i, carry):
            at = pl.ds(c * chunk_blocks + i * 2, 2)
            to = pl.ds(pl.multiple_of(i * sub, sub), sub)

            def values(j):
                held = mine[at] if j == 0 else others[j - 1, at]
                return held.astype(jnp.float32).reshape(sub, depth)

            row_sum = 0.0
            row_sq = 0.0
            for j in range(parts):
                x = values(j)
                row_sum = row_sum + jnp.sum(x, axis=1, keepdims=True)
                row_sq = row_sq + jnp.sum(x * x, axis=1, keepdims=True)
            mean = row_sum / width
            scale = lax.rsqrt(row_sq / width - mean * mean + EPS)
            for j in range(parts):
                cols = pl.ds(j * depth, depth)
                normed[to, cols] = ((values(j) - mean) * scale * gains[:, cols]).astype(
                    jnp.bfloat16
                )
            return carry

        lax.fori_loop(0, chunk // sub, norm_rows, 0)

        def columns(n, carry):
            cols = pl.ds(pl.multiple_of(n * tile, tile), tile)
            keys[pl.ds(base, chunk), cols] = jnp.dot(
                normed[...], weight[:, cols], preferred_element_type=jnp.float32
            ).astype(jnp.bfloat16)
            return carry

        lax.fori_loop(0, keys.shape[1] // tile, columns, 0)

        for i in range(per_chunk):
            step = c * per_chunk + i

            @pl.when(step < regular - 1)
            def _():
                key_copy(step).start()

        @pl.when(c == CHUNKS - 2)
        def _():
            local_copy(per_chunk).start()

        return carry

    lax.fori_loop(0, CHUNKS, one_chunk, 0)

    for i in range(per_chunk):
        local_copy(i).start()
    for i in range(per_chunk):
        early_copy(i).wait_send()
    for c in range(CHUNKS):
        for j in range(1, parts):
            gather_copy(c, j).wait_send()

    def finish(step, carry):
        key_copy(step).wait()
        return carry

    lax.fori_loop(0, regular - 1, finish, 0)
    for i in range(per_chunk + 1):
        local_copy(i).wait()


def on_device(groups, parts, memory_rows, norm_gain, key_weight, owner_table):
    row_count, depth = memory_rows.shape
    columns = key_weight.shape[1]
    blocks = row_count // BLK_ROWS
    capacity = blocks // groups
    any_space = pl.BlockSpec(memory_space=pl.ANY)
    in_vmem = pl.BlockSpec(memory_space=pltpu.VMEM)
    in_smem = pl.BlockSpec(memory_space=pltpu.SMEM)

    dma = pltpu.SemaphoreType.DMA
    listing = jax.ShapeDtypeStruct((groups, blocks), jnp.int32)
    slots, index = pl.pallas_call(
        functools.partial(index_kernel, groups, groups // CHUNKS),
        out_shape=[listing, listing],
        in_specs=[in_vmem],
        out_specs=[in_vmem, in_vmem],
        compiler_params=pltpu.CompilerParams(vmem_limit_bytes=4 * MIB),
        name="index",
    )(owner_table.reshape(groups, blocks))

    incoming = pl.pallas_call(
        functools.partial(main_kernel, groups, parts),
        out_shape=jax.ShapeDtypeStruct((row_count, columns), jnp.bfloat16),
        in_specs=[in_smem, any_space, any_space, any_space],
        out_specs=any_space,
        scratch_shapes=[
            pltpu.VMEM((blocks, BLK_ROWS, depth), jnp.bfloat16),
            pltpu.VMEM((blocks // CHUNKS, BLK_ROWS, depth), jnp.bfloat16),
            pltpu.VMEM((blocks, BLK_ROWS, depth), jnp.bfloat16),
            pltpu.VMEM((parts - 1, blocks, BLK_ROWS, depth), jnp.bfloat16),
            pltpu.VMEM((depth * parts, columns), jnp.bfloat16),
            pltpu.VMEM((row_count, columns), jnp.bfloat16),
            pltpu.VMEM((row_count // CHUNKS, depth * parts), jnp.bfloat16),
            pltpu.VMEM((1, depth * parts), jnp.float32),
            dma,
            dma((groups // CHUNKS,)),
            dma((groups // CHUNKS,)),
            dma((parts,)),
            dma((parts,)),
            dma((parts - 1, CHUNKS)),
            dma((parts - 1, CHUNKS)),
            dma((groups,)),
            dma((groups,)),
            dma((groups // CHUNKS + 1,)),
        ],
        compiler_params=pltpu.CompilerParams(
            collective_id=0, has_side_effects=True, vmem_limit_bytes=48 * MIB
        ),
        name="exchange",
    )(index, memory_rows.reshape(blocks, BLK_ROWS, depth), norm_gain[None, :], key_weight)

    placed = pl.pallas_call(
        functools.partial(place_kernel, groups),
        out_shape=jax.ShapeDtypeStruct((blocks, BLK_ROWS, columns), jnp.bfloat16),
        in_specs=[in_smem, in_vmem],
        out_specs=any_space,
        scratch_shapes=[pltpu.SemaphoreType.DMA],
        compiler_params=pltpu.CompilerParams(vmem_limit_bytes=16 * MIB),
        name="place",
    )(slots, incoming.reshape(blocks, BLK_ROWS, columns))
    return placed.reshape(row_count, columns)


def solution(mesh):
    in_specs = (P("grp", "tp"), P(), P(None, "tp"), P())
    out_specs = P("grp", "tp")
    return jax.shard_map(
        functools.partial(on_device, mesh.shape["grp"], mesh.shape["tp"]),
        mesh=mesh, in_specs=in_specs, out_specs=out_specs, check_vma=False,
    )
```

```python
import functools

import jax
import jax.numpy as jnp
from jax import lax
from jax.experimental import pallas as pl
from jax.experimental.pallas import tpu as pltpu
from jax.sharding import PartitionSpec as P

BLK_ROWS = 8
EPS = 1e-05
CHUNKS = 16
MIB = 1024 * 1024
MESH = pl.DeviceIdType.MESH


def flipped(me, mask, groups):
    out = me
    bit = 1
    while bit < groups:
        out = out + ((mask // bit) % 2) * bit * (1 - 2 * ((me // bit) % 2))
        bit *= 2
    return out


def mask_at(me, step, groups):
    quarter = groups // 4
    inner = ((me // quarter + 1) // 2) % 2
    turn = step // quarter
    first = (3 - turn) // 3
    second = (turn % 2) * (1 - turn // 2)
    third = (turn // 2) * (1 - turn % 2)
    far = first * (1 + inner) + 3 * second + third * (2 - inner)
    return far * quarter + quarter - 1 - step % quarter


def peer_mask(me, step, groups, early):
    regular = groups - early
    split = groups // 2 - early
    is_early = step // regular
    after = (1 + step // split) // 2
    late = step - regular + split
    return mask_at(me, is_early * late + (1 - is_early) * (step + early * after), groups)


def index_kernel(groups, per_chunk, table_ref, slot_ref, index_ref):
    me = lax.axis_index("grp")
    blocks = table_ref.shape[1]
    capacity = blocks // groups

    lane = lax.broadcasted_iota(jnp.int32, (groups, blocks), 1)
    row = lax.broadcasted_iota(jnp.int32, (groups, blocks), 0)
    peer = jnp.zeros((groups, blocks), jnp.int32)
    for step in range(groups):
        mask = peer_mask(me, step, groups, per_chunk)
        peer = jnp.where(row == step, flipped(me, mask, groups), peer)

    def ranked(offset, value):
        chosen = (offset >= 0) & (offset < blocks)
        counted = chosen.astype(jnp.int32)
        shift = 1
        while shift < blocks:
            counted = counted + jnp.where(lane >= shift, pltpu.roll(counted, shift, 1), 0)
            shift *= 2
        result = jnp.zeros((groups, blocks), jnp.int32)
        for r in range(capacity):
            at_rank = jnp.where(chosen & (counted == r + 1), value, 0).astype(jnp.float32)
            found = jnp.sum(at_rank, axis=1, keepdims=True).astype(jnp.int32)
            result = jnp.where(lane == r, found, result)
        return result

    own = jnp.broadcast_to(table_ref[pl.ds(me, 1), :], (groups, blocks))
    index_ref[...] = ranked(own - peer * blocks, lane)
    offset = table_ref[...] - me * blocks
    slot_ref[...] = ranked(offset, offset)


def place_kernel(groups, slot_ref, in_ref, out_ref, sem):
    me = lax.axis_index("grp")
    blocks = in_ref.shape[0]
    capacity = blocks // groups

    def move(i, carry):
        mask = i // capacity
        slot = slot_ref[me ^ mask, i - mask * capacity]
        pltpu.make_async_copy(in_ref.at[i], out_ref.at[slot], sem).start()
        return carry

    lax.fori_loop(0, blocks, move, 0, unroll=8)
    pltpu.make_async_copy(in_ref, out_ref, sem).wait()


def main_kernel(
    groups, parts, index_ref, rows_ref, gain_ref, weight_ref, out_ref,
    raw, away, mine, others, weight, keys, normed, gains,
    raw_sem, early_send, early_recv, weight_sem, gain_sem, gather_send, gather_recv, key_send, key_recv, self_sem,
):
    me = lax.axis_index("grp")
    part = lax.axis_index("tp")
    blocks, _, depth = rows_ref.shape
    row_count = blocks * BLK_ROWS
    width = depth * parts
    chunk = row_count // CHUNKS
    chunk_blocks = blocks // CHUNKS
    capacity = blocks // groups
    per_chunk = groups // CHUNKS
    piece = row_count // groups
    regular = groups - per_chunk

    barrier = pltpu.get_barrier_semaphore()
    def greet(i, carry):
        mask = groups - i
        pl.semaphore_signal(
            barrier, inc=1, device_id={"grp": flipped(me, mask, groups)}, device_id_type=MESH
        )
        return carry

    lax.fori_loop(1, groups, greet, 0)
    for j in range(1, parts):
        pl.semaphore_signal(
            barrier, inc=1, device_id={"tp": (part + j) % parts}, device_id_type=MESH
        )

    raw_copy = pltpu.make_async_copy(rows_ref, raw, raw_sem)

    def weight_copy(j):
        origin = (part + j) % parts
        return pltpu.make_async_copy(
            weight_ref.at[pl.ds(pl.multiple_of(origin * depth, depth), depth)],
            weight.at[pl.ds(j * depth, depth)],
            weight_sem.at[j],
        )

    def gain_copy(j):
        origin = (part + j) % parts
        return pltpu.make_async_copy(
            gain_ref.at[:, pl.ds(pl.multiple_of(origin * depth, depth), depth)],
            gains.at[:, pl.ds(j * depth, depth)],
            gain_sem.at[j],
        )

    def gather_copy(c, j):
        at = pl.ds(c * chunk_blocks, chunk_blocks)
        return pltpu.make_async_remote_copy(
            src_ref=mine.at[at],
            dst_ref=others.at[j - 1, at],
            send_sem=gather_send.at[j - 1, c],
            recv_sem=gather_recv.at[j - 1, c],
            device_id={"tp": (part + parts - j) % parts},
            device_id_type=MESH,
        )

    def key_copy(step):
        mask = peer_mask(me, step, groups, per_chunk)
        return pltpu.make_async_remote_copy(
            src_ref=keys.at[pl.ds(step * piece, piece)],
            dst_ref=out_ref.at[pl.ds(mask * piece, piece)],
            send_sem=key_send.at[step],
            recv_sem=key_recv.at[mask],
            device_id={"grp": flipped(me, mask, groups)},
            device_id_type=MESH,
        )

    def local_copy(i):
        step = regular + i if i < per_chunk else regular - 1
        mask = peer_mask(me, step, groups, per_chunk)
        return pltpu.make_async_copy(
            keys.at[pl.ds(step * piece, piece)],
            out_ref.at[pl.ds(mask * piece, piece)],
            self_sem.at[i],
        )

    def early_copy(i):
        mask = peer_mask(me, regular + i, groups, per_chunk)
        return pltpu.make_async_remote_copy(
            src_ref=away.at[pl.ds(i * capacity, capacity)],
            dst_ref=mine.at[pl.ds((regular + i) * capacity, capacity)],
            send_sem=early_send.at[i],
            recv_sem=early_recv.at[i],
            device_id={"grp": flipped(me, mask, groups)},
            device_id_type=MESH,
        )

    raw_copy.start()

    for j in range(parts):
        gain_copy(j).start()
    raw_copy.wait()
    for j in range(parts):
        weight_copy(j).start()

    def arrange(c):
        def take(i, carry):
            step = i // capacity
            block = raw[index_ref[step, i - step * capacity]]
            if c == CHUNKS - 1:
                away[i - c * chunk_blocks] = block
            else:
                mine[i] = block
            return carry

        lax.fori_loop(c * chunk_blocks, (c + 1) * chunk_blocks, take, 0)

    arrange(CHUNKS - 1)
    arrange(0)
    pl.semaphore_wait(barrier, groups - 1 + parts - 1)
    for i in range(per_chunk):
        early_copy(i).start()
    for c in range(CHUNKS - 1):
        if c > 0:
            arrange(c)
        for j in range(1, parts):
            gather_copy(c, j).start()
    for j in range(parts):
        gain_copy(j).wait()
        weight_copy(j).wait()

    sub = 2 * BLK_ROWS
    tile = depth // 2

    def one_chunk(c, carry):
        base = pl.multiple_of(c * chunk, chunk)

        @pl.when(c == CHUNKS // 2)
        def _():
            for i in range(per_chunk):
                early_copy(i).wait_recv()
            for j in range(1, parts):
                gather_copy(CHUNKS - 1, j).start()

        for j in range(1, parts):
            gather_copy(c, j).wait_recv()

        def norm_rows(i, carry):
            at = pl.ds(c * chunk_blocks + i * 2, 2)
            to = pl.ds(pl.multiple_of(i * sub, sub), sub)

            def values(j):
                held = mine[at] if j == 0 else others[j - 1, at]
                return held.astype(jnp.float32).reshape(sub, depth)

            row_sum = 0.0
            row_sq = 0.0
            for j in range(parts):
                x = values(j)
                row_sum = row_sum + jnp.sum(x, axis=1, keepdims=True)
                row_sq = row_sq + jnp.sum(x * x, axis=1, keepdims=True)
            mean = row_sum / width
            scale = lax.rsqrt(row_sq / width - mean * mean + EPS)
            for j in range(parts):
                cols = pl.ds(j * depth, depth)
                normed[to, cols] = ((values(j) - mean) * scale * gains[:, cols]).astype(
                    jnp.bfloat16
                )
            return carry

        lax.fori_loop(0, chunk // sub, norm_rows, 0)

        def columns(n, carry):
            cols = pl.ds(pl.multiple_of(n * tile, tile), tile)
            keys[pl.ds(base, chunk), cols] = jnp.dot(
                normed[...], weight[:, cols], preferred_element_type=jnp.float32
            ).astype(jnp.bfloat16)
            return carry

        lax.fori_loop(0, keys.shape[1] // tile, columns, 0)

        for i in range(per_chunk):
            step = c * per_chunk + i

            @pl.when(step < regular - 1)
            def _():
                key_copy(step).start()

        @pl.when(c == CHUNKS - 2)
        def _():
            local_copy(per_chunk).start()

        return carry

    lax.fori_loop(0, CHUNKS, one_chunk, 0)

    for i in range(per_chunk):
        local_copy(i).start()
    for i in range(per_chunk):
        early_copy(i).wait_send()
    for c in range(CHUNKS):
        for j in range(1, parts):
            gather_copy(c, j).wait_send()

    def finish(step, carry):
        key_copy(step).wait()
        return carry

    lax.fori_loop(0, regular - 1, finish, 0)
    for i in range(per_chunk + 1):
        local_copy(i).wait()


def on_device(groups, parts, memory_rows, norm_gain, key_weight, owner_table):
    row_count, depth = memory_rows.shape
    columns = key_weight.shape[1]
    blocks = row_count // BLK_ROWS
    capacity = blocks // groups
    any_space = pl.BlockSpec(memory_space=pl.ANY)
    in_hbm = pl.BlockSpec(memory_space=pltpu.HBM)
    in_vmem = pl.BlockSpec(memory_space=pltpu.VMEM)
    in_smem = pl.BlockSpec(memory_space=pltpu.SMEM)

    dma = pltpu.SemaphoreType.DMA
    listing = jax.ShapeDtypeStruct((groups, blocks), jnp.int32)
    slots, index = pl.pallas_call(
        functools.partial(index_kernel, groups, groups // CHUNKS),
        out_shape=[listing, listing],
        in_specs=[in_vmem],
        out_specs=[in_vmem, in_vmem],
        compiler_params=pltpu.CompilerParams(vmem_limit_bytes=4 * MIB),
        name="index",
    )(owner_table.reshape(groups, blocks))

    incoming = pl.pallas_call(
        functools.partial(main_kernel, groups, parts),
        out_shape=jax.ShapeDtypeStruct((row_count, columns), jnp.bfloat16),
        in_specs=[in_smem, in_hbm, in_hbm, in_hbm],
        out_specs=any_space,
        scratch_shapes=[
            pltpu.VMEM((blocks, BLK_ROWS, depth), jnp.bfloat16),
            pltpu.VMEM((blocks // CHUNKS, BLK_ROWS, depth), jnp.bfloat16),
            pltpu.VMEM((blocks, BLK_ROWS, depth), jnp.bfloat16),
            pltpu.VMEM((parts - 1, blocks, BLK_ROWS, depth), jnp.bfloat16),
            pltpu.VMEM((depth * parts, columns), jnp.bfloat16),
            pltpu.VMEM((row_count, columns), jnp.bfloat16),
            pltpu.VMEM((row_count // CHUNKS, depth * parts), jnp.bfloat16),
            pltpu.VMEM((1, depth * parts), jnp.float32),
            dma,
            dma((groups // CHUNKS,)),
            dma((groups // CHUNKS,)),
            dma((parts,)),
            dma((parts,)),
            dma((parts - 1, CHUNKS)),
            dma((parts - 1, CHUNKS)),
            dma((groups,)),
            dma((groups,)),
            dma((groups // CHUNKS + 1,)),
        ],
        compiler_params=pltpu.CompilerParams(
            collective_id=0, has_side_effects=True, vmem_limit_bytes=48 * MIB
        ),
        name="exchange",
    )(index, memory_rows.reshape(blocks, BLK_ROWS, depth), norm_gain[None, :], key_weight)

    placed = pl.pallas_call(
        functools.partial(place_kernel, groups),
        out_shape=jax.ShapeDtypeStruct((blocks, BLK_ROWS, columns), jnp.bfloat16),
        in_specs=[in_smem, in_vmem],
        out_specs=any_space,
        scratch_shapes=[pltpu.SemaphoreType.DMA],
        compiler_params=pltpu.CompilerParams(vmem_limit_bytes=16 * MIB),
        name="place",
    )(slots, incoming.reshape(blocks, BLK_ROWS, columns))
    return placed.reshape(row_count, columns)


def solution(mesh):
    in_specs = (P("grp", "tp"), P(), P(None, "tp"), P())
    out_specs = P("grp", "tp")
    return jax.shard_map(
        functools.partial(on_device, mesh.shape["grp"], mesh.shape["tp"]),
        mesh=mesh, in_specs=in_specs, out_specs=out_specs, check_vma=False,
    )
```

```python
import functools

import jax
import jax.numpy as jnp
from jax import lax
from jax.experimental import pallas as pl
from jax.experimental.pallas import tpu as pltpu
from jax.sharding import PartitionSpec as P

BLK_ROWS = 8
EPS = 1e-05
CHUNKS = 16
MIB = 1024 * 1024
MESH = pl.DeviceIdType.MESH


def flipped(me, mask, groups):
    out = me
    bit = 1
    while bit < groups:
        out = out + ((mask // bit) % 2) * bit * (1 - 2 * ((me // bit) % 2))
        bit *= 2
    return out


def mask_at(me, step, groups):
    quarter = groups // 4
    inner = ((me // quarter + 1) // 2) % 2
    turn = step // quarter
    first = (3 - turn) // 3
    second = (turn % 2) * (1 - turn // 2)
    third = (turn // 2) * (1 - turn % 2)
    far = first * (1 + inner) + 3 * second + third * (2 - inner)
    return far * quarter + quarter - 1 - step % quarter


def peer_mask(me, step, groups, early):
    regular = groups - early
    split = groups // 2 - early
    is_early = step // regular
    after = (1 + step // split) // 2
    late = step - regular + split
    return mask_at(me, is_early * late + (1 - is_early) * (step + early * after), groups)


def index_kernel(groups, per_chunk, table_ref, slot_ref, index_ref):
    me = lax.axis_index("grp")
    blocks = table_ref.shape[1]
    capacity = blocks // groups

    lane = lax.broadcasted_iota(jnp.int32, (groups, blocks), 1)
    row = lax.broadcasted_iota(jnp.int32, (groups, blocks), 0)
    peer = jnp.zeros((groups, blocks), jnp.int32)
    for step in range(groups):
        mask = peer_mask(me, step, groups, per_chunk)
        peer = jnp.where(row == step, flipped(me, mask, groups), peer)

    def ranked(offset, value):
        chosen = (offset >= 0) & (offset < blocks)
        counted = chosen.astype(jnp.int32)
        shift = 1
        while shift < blocks:
            counted = counted + jnp.where(lane >= shift, pltpu.roll(counted, shift, 1), 0)
            shift *= 2
        result = jnp.zeros((groups, blocks), jnp.int32)
        for r in range(capacity):
            at_rank = jnp.where(chosen & (counted == r + 1), value, 0).astype(jnp.float32)
            found = jnp.sum(at_rank, axis=1, keepdims=True).astype(jnp.int32)
            result = jnp.where(lane == r, found, result)
        return result

    own = jnp.broadcast_to(table_ref[pl.ds(me, 1), :], (groups, blocks))
    index_ref[...] = ranked(own - peer * blocks, lane)
    offset = table_ref[...] - me * blocks
    slot_ref[...] = ranked(offset, offset)


def place_kernel(groups, slot_ref, in_ref, out_ref, sem):
    me = lax.axis_index("grp")
    blocks = in_ref.shape[0]
    capacity = blocks // groups

    def move(i, carry):
        mask = i // capacity
        slot = slot_ref[me ^ mask, i - mask * capacity]
        pltpu.make_async_copy(in_ref.at[i], out_ref.at[slot], sem).start()
        return carry

    lax.fori_loop(0, blocks, move, 0, unroll=8)
    pltpu.make_async_copy(in_ref, out_ref, sem).wait()


def main_kernel(
    groups, parts, index_ref, rows_ref, gain_ref, weight_ref, out_ref,
    raw, away, mine, others, weight, keys, normed, gains,
    raw_sem, early_send, early_recv, weight_sem, gain_sem, gather_send, gather_recv, key_send, key_recv, self_sem,
):
    me = lax.axis_index("grp")
    part = lax.axis_index("tp")
    blocks, _, depth = rows_ref.shape
    row_count = blocks * BLK_ROWS
    width = depth * parts
    chunk = row_count // CHUNKS
    chunk_blocks = blocks // CHUNKS
    capacity = blocks // groups
    per_chunk = groups // CHUNKS
    piece = row_count // groups
    regular = groups - per_chunk

    barrier = pltpu.get_barrier_semaphore()
    def greet(i, carry):
        mask = groups - i
        pl.semaphore_signal(
            barrier, inc=1, device_id={"grp": flipped(me, mask, groups)}, device_id_type=MESH
        )
        return carry

    lax.fori_loop(1, groups, greet, 0)
    for j in range(1, parts):
        pl.semaphore_signal(
            barrier, inc=1, device_id={"tp": (part + j) % parts}, device_id_type=MESH
        )

    raw_copy = pltpu.make_async_copy(rows_ref, raw, raw_sem)

    def weight_copy(j):
        origin = (part + j) % parts
        return pltpu.make_async_copy(
            weight_ref.at[pl.ds(pl.multiple_of(origin * depth, depth), depth)],
            weight.at[pl.ds(j * depth, depth)],
            weight_sem.at[j],
        )

    def gain_copy(j):
        origin = (part + j) % parts
        return pltpu.make_async_copy(
            gain_ref.at[:, pl.ds(pl.multiple_of(origin * depth, depth), depth)],
            gains.at[:, pl.ds(j * depth, depth)],
            gain_sem.at[j],
        )

    def gather_copy(c, j):
        at = pl.ds(c * chunk_blocks, chunk_blocks)
        return pltpu.make_async_remote_copy(
            src_ref=mine.at[at],
            dst_ref=others.at[j - 1, at],
            send_sem=gather_send.at[j - 1, c],
            recv_sem=gather_recv.at[j - 1, c],
            device_id={"tp": (part + parts - j) % parts},
            device_id_type=MESH,
        )

    def key_copy(step):
        mask = peer_mask(me, step, groups, per_chunk)
        return pltpu.make_async_remote_copy(
            src_ref=keys.at[pl.ds(step * piece, piece)],
            dst_ref=out_ref.at[pl.ds(mask * piece, piece)],
            send_sem=key_send.at[step],
            recv_sem=key_recv.at[mask],
            device_id={"grp": flipped(me, mask, groups)},
            device_id_type=MESH,
        )

    def local_copy(i):
        step = regular + i if i < per_chunk else regular - 1
        mask = peer_mask(me, step, groups, per_chunk)
        return pltpu.make_async_copy(
            keys.at[pl.ds(step * piece, piece)],
            out_ref.at[pl.ds(mask * piece, piece)],
            self_sem.at[i],
        )

    def early_copy(i):
        mask = peer_mask(me, regular + i, groups, per_chunk)
        return pltpu.make_async_remote_copy(
            src_ref=away.at[pl.ds(i * capacity, capacity)],
            dst_ref=mine.at[pl.ds((regular + i) * capacity, capacity)],
            send_sem=early_send.at[i],
            recv_sem=early_recv.at[i],
            device_id={"grp": flipped(me, mask, groups)},
            device_id_type=MESH,
        )

    raw_copy.start()

    for j in range(parts):
        gain_copy(j).start()
    raw_copy.wait()
    for j in range(parts):
        weight_copy(j).start()

    def arrange(c):
        def take(i, carry):
            step = i // capacity
            block = raw[index_ref[step, i - step * capacity]]
            if c == CHUNKS - 1:
                away[i - c * chunk_blocks] = block
            else:
                mine[i] = block
            return carry

        lax.fori_loop(c * chunk_blocks, (c + 1) * chunk_blocks, take, 0, unroll=2)

    arrange(0)
    pl.semaphore_wait(barrier, groups - 1 + parts - 1)
    for c in range(CHUNKS - 1):
        if c > 0:
            arrange(c)
        for j in range(1, parts):
            gather_copy(c, j).start()
        if c == 0:
            arrange(CHUNKS - 1)
            for i in range(per_chunk):
                early_copy(i).start()
    for j in range(parts):
        gain_copy(j).wait()
        weight_copy(j).wait()

    sub = 2 * BLK_ROWS
    tile = depth

    def one_chunk(c, carry):
        base = pl.multiple_of(c * chunk, chunk)

        @pl.when(c == CHUNKS // 2)
        def _():
            for i in range(per_chunk):
                early_copy(i).wait_recv()
            for j in range(1, parts):
                gather_copy(CHUNKS - 1, j).start()

        for j in range(1, parts):
            gather_copy(c, j).wait_recv()

        def norm_rows(i, carry):
            at = pl.ds(c * chunk_blocks + i * 2, 2)
            to = pl.ds(pl.multiple_of(i * sub, sub), sub)

            def values(j):
                held = mine[at] if j == 0 else others[j - 1, at]
                return held.astype(jnp.float32).reshape(sub, depth)

            row_sum = 0.0
            row_sq = 0.0
            for j in range(parts):
                x = values(j)
                row_sum = row_sum + jnp.sum(x, axis=1, keepdims=True)
                row_sq = row_sq + jnp.sum(x * x, axis=1, keepdims=True)
            mean = row_sum / width
            scale = lax.rsqrt(row_sq / width - mean * mean + EPS)
            for j in range(parts):
                cols = pl.ds(j * depth, depth)
                normed[to, cols] = ((values(j) - mean) * scale * gains[:, cols]).astype(
                    jnp.bfloat16
                )
            return carry

        lax.fori_loop(0, chunk // sub, norm_rows, 0)

        def columns(n, carry):
            cols = pl.ds(pl.multiple_of(n * tile, tile), tile)
            keys[pl.ds(base, chunk), cols] = jnp.dot(
                normed[...], weight[:, cols], preferred_element_type=jnp.float32
            ).astype(jnp.bfloat16)
            return carry

        lax.fori_loop(0, keys.shape[1] // tile, columns, 0)

        for i in range(per_chunk):
            step = c * per_chunk + i

            @pl.when(step < regular - 1)
            def _():
                key_copy(step).start()

        @pl.when(c == CHUNKS - 2)
        def _():
            local_copy(per_chunk).start()

        return carry

    lax.fori_loop(0, CHUNKS, one_chunk, 0)

    for i in range(per_chunk):
        local_copy(i).start()
    for i in range(per_chunk):
        early_copy(i).wait_send()
    for c in range(CHUNKS):
        for j in range(1, parts):
            gather_copy(c, j).wait_send()

    def finish(step, carry):
        key_copy(step).wait()
        return carry

    lax.fori_loop(0, regular - 1, finish, 0)
    for i in range(per_chunk + 1):
        local_copy(i).wait()


def on_device(groups, parts, memory_rows, norm_gain, key_weight, owner_table):
    row_count, depth = memory_rows.shape
    columns = key_weight.shape[1]
    blocks = row_count // BLK_ROWS
    capacity = blocks // groups
    any_space = pl.BlockSpec(memory_space=pl.ANY)
    in_hbm = pl.BlockSpec(memory_space=pltpu.HBM)
    in_vmem = pl.BlockSpec(memory_space=pltpu.VMEM)
    in_smem = pl.BlockSpec(memory_space=pltpu.SMEM)

    dma = pltpu.SemaphoreType.DMA
    listing = jax.ShapeDtypeStruct((groups, blocks), jnp.int32)
    slots, index = pl.pallas_call(
        functools.partial(index_kernel, groups, groups // CHUNKS),
        out_shape=[listing, listing],
        in_specs=[in_vmem],
        out_specs=[in_vmem, in_vmem],
        compiler_params=pltpu.CompilerParams(vmem_limit_bytes=4 * MIB),
        name="index",
    )(owner_table.reshape(groups, blocks))

    incoming = pl.pallas_call(
        functools.partial(main_kernel, groups, parts),
        out_shape=jax.ShapeDtypeStruct((row_count, columns), jnp.bfloat16),
        in_specs=[in_smem, in_hbm, in_hbm, in_hbm],
        out_specs=any_space,
        scratch_shapes=[
            pltpu.VMEM((blocks, BLK_ROWS, depth), jnp.bfloat16),
            pltpu.VMEM((blocks // CHUNKS, BLK_ROWS, depth), jnp.bfloat16),
            pltpu.VMEM((blocks, BLK_ROWS, depth), jnp.bfloat16),
            pltpu.VMEM((parts - 1, blocks, BLK_ROWS, depth), jnp.bfloat16),
            pltpu.VMEM((depth * parts, columns), jnp.bfloat16),
            pltpu.VMEM((row_count, columns), jnp.bfloat16),
            pltpu.VMEM((row_count // CHUNKS, depth * parts), jnp.bfloat16),
            pltpu.VMEM((1, depth * parts), jnp.float32),
            dma,
            dma((groups // CHUNKS,)),
            dma((groups // CHUNKS,)),
            dma((parts,)),
            dma((parts,)),
            dma((parts - 1, CHUNKS)),
            dma((parts - 1, CHUNKS)),
            dma((groups,)),
            dma((groups,)),
            dma((groups // CHUNKS + 1,)),
        ],
        compiler_params=pltpu.CompilerParams(
            collective_id=0, has_side_effects=True, vmem_limit_bytes=48 * MIB
        ),
        name="exchange",
    )(index, memory_rows.reshape(blocks, BLK_ROWS, depth), norm_gain[None, :], key_weight)

    placed = pl.pallas_call(
        functools.partial(place_kernel, groups),
        out_shape=jax.ShapeDtypeStruct((blocks, BLK_ROWS, columns), jnp.bfloat16),
        in_specs=[in_smem, in_vmem],
        out_specs=any_space,
        scratch_shapes=[pltpu.SemaphoreType.DMA],
        compiler_params=pltpu.CompilerParams(vmem_limit_bytes=16 * MIB),
        name="place",
    )(slots, incoming.reshape(blocks, BLK_ROWS, columns))
    return placed.reshape(row_count, columns)


def solution(mesh):
    in_specs = (P("grp", "tp"), P(), P(None, "tp"), P())
    out_specs = P("grp", "tp")
    return jax.shard_map(
        functools.partial(on_device, mesh.shape["grp"], mesh.shape["tp"]),
        mesh=mesh, in_specs=in_specs, out_specs=out_specs, check_vma=False,
    )
```
